32 devices in a mesh: pipe: 2 (over x), tensor: 2 (over core), dp: 8 (over z, y).
Axes of the slice: x: 2, y: 2, z: 4, core: 2. Of those that a mesh axis runs over, the one named last changes fastest.
Arguments:
- attn_out: bfloat16 [2, 4, 1024, 4096], P('pipe', None, 'dp', 'tensor'), may hold values from -6 to 6
- grad_top: bfloat16 [4, 1024, 4096], P(None, 'dp', 'tensor'), may hold values from -6 to 6
- branch_grad: bfloat16 [2, 4, 1024, 4096], P('pipe', None, 'dp', 'tensor'), may hold values from -6 to 6
- error_prev: bfloat16 [2, 8, 4096, 4096], P('pipe', 'dp', 'tensor'), may hold values from -0.3984375 to 0.3984375
- q_prev: float32 [2, 4096, 64], P('pipe', 'tensor'), may hold values from -6 to 6
Outputs:
- grad_input: bfloat16 [2, 4, 1024, 4096], P('pipe', None, 'dp', 'tensor')
- error_next: bfloat16 [2, 8, 4096, 4096], P('pipe', 'dp', 'tensor')
- p_factor: float32 [2, 4096, 64], P('pipe', 'tensor')
- q_factor: float32 [2, 4096, 64], P('pipe', 'tensor')
The draws below stay inside these ranges and needn't reach their ends.
All inputs are finite; a program needn't handle non-finite values.
Results may differ from the reference program's by a relative error of at most 0.012.
Values may be sent and summed in bfloat16 or wider, within the bound.
A program may use at most 256 MiB of HBM per device.

```python
import jax
import jax.numpy as jnp
from jax import lax

D = 4096
RANK = 64
MB = 4
TOK_MB = 128
TOKS = 1024
HDALL = 4096
N_PIPE = 2
N_DP = 8


def shard_levels(stream_key, extent, shards, smallest, top_value):
    factor_of = 1.0
    for position, parts in shards:
        heights = jax.random.uniform(jax.random.fold_in(jax.random.fold_in(stream_key, 6), position), (parts,), jnp.float32, smallest / len(shards), top_value / len(shards))
        factor_of = factor_of * jnp.repeat(jnp.exp(heights), extent[position] // parts).reshape((-1,) + (1,) * (len(extent) - 1 - position))
    return factor_of


def noise(rng, shape, deviation, bound, pieces=(), held_as=jnp.bfloat16):
    drawn = deviation * jax.random.normal(rng, shape, jnp.float32)
    if pieces:
        drawn = drawn * shard_levels(rng, shape, pieces, -0.22, 0.18)
    return jnp.clip(drawn, -bound, bound).astype(held_as)


def setup_inputs(seed: int = 0) -> dict:
    splits = jax.random.split(jax.random.key(seed), 6)
    return {
        "attn_out": noise(splits[0], (N_PIPE, MB, TOKS, HDALL), 1.0, 6.0, ((0, 2), (2, 8), (3, 2))),
        "grad_top": noise(splits[1], (MB, TOKS, D), 1.0, 6.0, ((1, 8), (2, 2))),
        "branch_grad": noise(splits[2], (N_PIPE, MB, TOKS, D), 1.0, 6.0, ((0, 2), (2, 8), (3, 2))),
        "error_prev": noise(splits[3], (N_PIPE, N_DP, HDALL, D), 0.05, 0.3984375, ((0, 2), (1, 8), (2, 2))),
        "q_prev": noise(splits[4], (N_PIPE, D, RANK), 1.0, 6.0, ((0, 2), (1, 2)), jnp.float32),
    }


def orthonormal(praw):
    gram = jnp.dot(praw.T, praw, precision=lax.Precision.HIGHEST)
    lower = jnp.linalg.cholesky(gram)
    return lax.linalg.triangular_solve(lower, praw, left_side=False, lower=True, transpose_a=True)

def reference(attn_out, grad_top, branch_grad, error_prev, q_prev):
    scale = 1.0 / (MB * TOK_MB)
    high = lax.Precision.HIGHEST
    out_grad = grad_top
    inputs, errors, pfacts, qfacts = ([], [], [], [])
    for section in reversed(range(N_PIPE)):
        grad_in = (out_grad.astype(jnp.float32) + branch_grad[section].astype(jnp.float32)).astype(jnp.bfloat16)
        acts = attn_out[section].reshape(MB, N_DP, TOK_MB, HDALL).transpose(1, 0, 2, 3)
        grads = out_grad.reshape(MB, N_DP, TOK_MB, D).transpose(1, 0, 2, 3)

        def local(triple):
            act_rep, grad_rep, err_rep = triple
            total = jnp.zeros((HDALL, D), jnp.float32)
            for micro in range(MB):
                total = total + jnp.dot(act_rep[micro].T.astype(jnp.float32), grad_rep[micro].astype(jnp.float32), preferred_element_type=jnp.float32)
            return total * scale + err_rep.astype(jnp.float32)
        mats = lax.map(local, (acts, grads, error_prev[section]))
        qold = q_prev[section]
        praw = jnp.sum(lax.map(lambda mat: jnp.dot(mat, qold, precision=high), mats), axis=0) / N_DP
        phat = orthonormal(praw)
        qnew = jnp.sum(lax.map(lambda mat: jnp.dot(mat.T, phat, precision=high), mats), axis=0) / N_DP
        err = lax.map(lambda mat: (mat - jnp.dot(phat, qnew.T, precision=high)).astype(jnp.bfloat16), mats)
        inputs.insert(0, grad_in)
        errors.insert(0, err)
        pfacts.insert(0, phat)
        qfacts.insert(0, qnew)
        out_grad = grad_in
    return (jnp.stack(inputs), jnp.stack(errors), jnp.stack(pfacts), jnp.stack(qfacts))
```

```python
import functools

import jax
import jax.numpy as jnp
from jax import lax
from jax.experimental import pallas as pl
from jax.experimental.pallas import tpu as pltpu
from jax.sharding import PartitionSpec as P

BF16 = jnp.bfloat16
F32 = jnp.float32
NN = (((1,), (0,)), ((), ()))
NT = (((1,), (1,)), ((), ()))
TN = (((0,), (0,)), ((), ()))


def mm(a, b, dims):
    return lax.dot_general(a, b, dims, preferred_element_type=F32)


def terms(x):
    head = x.astype(BF16)
    tail = (x - head.astype(F32)).astype(BF16)
    return jnp.concatenate([head, tail], axis=0)


def fold(y):
    half = y.shape[0] // 2
    return y[:half] + y[half:]


def add_round(a, b):
    return (a.astype(F32) + b.astype(F32)).astype(BF16)


def inverse_factor(gram):
    rank = gram.shape[0]
    row = lax.broadcasted_iota(jnp.int32, (rank, 2 * rank), 0)
    col = lax.broadcasted_iota(jnp.int32, (rank, 2 * rank), 1)
    work = jnp.concatenate([gram, jnp.where(row == col, 1.0, 0.0)[:, :rank]], axis=1)
    for k in range(rank - 1):
        ratio = work[:, k : k + 1] * (1.0 / work[k : k + 1, k : k + 1])
        work = work - jnp.where(row > k, ratio * work[k : k + 1, :], 0.0)
    diagonal = jnp.sum(jnp.where(row == col, work, 0.0), axis=1, keepdims=True)
    return work[:, rank:] * lax.rsqrt(diagonal)


class Semaphores:
    def __init__(self):
        self.count = 0

    def take(self, n=1):
        first = self.count
        self.count += n
        return first


def semaphore_map(tensor, dp, bulk, tiles):
    s = Semaphores()
    names = {}
    for name, n in (
        ("err", tiles), ("g_out", 1),
        ("q_s", tensor), ("q_r", tensor), ("q0_s", 1), ("q0_r", 1),
        ("bulk_s", bulk), ("bulk_r", bulk), ("gx_s", 1), ("gx_r", 1),
        ("gq_s", tensor), ("gq_r", tensor), ("p_s", dp), ("p_r", dp),
        ("pg_s", dp), ("pg_r", dp), ("gram_s", tensor), ("gram_r", tensor),
        ("ap_s", tensor), ("ap_r", tensor), ("qx_s", tensor), ("qx_r", tensor),
        ("g_s", tensor), ("g_r", tensor), ("qp_s", dp), ("qp_r", dp),
        ("qg_s", dp), ("qg_r", dp), ("qf_s", tensor * dp), ("qf_r", tensor * dp),
    ):
        names[name] = s.take(n)
    return names, s.count


def chain_kernel(
    dims, attn, gtop, branch, err_hbm, q_in,
    g_out, p_out, q_out, q_own,
    err, qg, q0, gadd, land, gbuf, gqx, gqb, eq, psend, prcv, pg, praw, gb,
    phl, apb, qx, qxr, qsend, qrcv, qf, sem,
):
    tensor, dp, bulk, tiles, names = dims
    tokens, head_rows = attn.shape
    features = gtop.shape[1]
    rank = q_in.shape[0]
    pw, qw = head_rows // dp, features // dp
    section = lax.axis_index("pipe")
    t = lax.axis_index("tensor")
    r = lax.axis_index("dp")
    scale = 1.0 / tokens

    def at(name, index=0):
        return sem.at[names[name] + index]

    def remote(src, dst, send, recv, **where):
        return pltpu.make_async_remote_copy(
            src_ref=src, dst_ref=dst, send_sem=send, recv_sem=recv,
            device_id=where, device_id_type=pl.DeviceIdType.MESH,
        )

    tensor_peers = [lax.rem(t + o, tensor) for o in range(1, tensor)]
    dp_peers = [lax.rem(r + o, dp) for o in range(1, dp)]

    def over_tensor(src, dst, key):
        return [
            remote(src, dst.at[t], at(key + "_s", o), at(key + "_r", t), tensor=peer)
            for o, peer in enumerate(tensor_peers)
        ]

    def from_tensor(dst, key):
        for peer in tensor_peers:
            remote(dst.at[peer], dst.at[peer], at(key + "_s"), at(key + "_r", peer), tensor=peer).wait_recv()

    def over_dp(src_of, dst, key):
        return [
            remote(src_of(peer), dst.at[r], at(key + "_s", o), at(key + "_r", r), dp=peer)
            for o, peer in enumerate(dp_peers)
        ]

    def from_dp(dst, key):
        for peer in dp_peers:
            remote(dst.at[peer], dst.at[peer], at(key + "_s"), at(key + "_r", peer), dp=peer).wait_recv()

    def start(copies):
        for copy in copies:
            copy.start()

    def sent(copies):
        for copy in copies:
            copy.wait_send()

    tile = head_rows // tiles

    def err_copy(i):
        rows = pl.ds(pl.multiple_of(i * tile, tile), tile)
        return pltpu.make_async_copy(err_hbm.at[rows], err.at[rows], at("err", i))

    for i in range(tiles):
        err_copy(i).start()
    qg[t] = terms(q_in[...])

    barrier = pltpu.get_barrier_semaphore()
    for peer in tensor_peers:
        pl.semaphore_signal(barrier, inc=1, device_id={"tensor": peer}, device_id_type=pl.DeviceIdType.MESH)
    for peer in dp_peers:
        pl.semaphore_signal(barrier, inc=1, device_id={"dp": peer}, device_id_type=pl.DeviceIdType.MESH)
    pl.semaphore_signal(barrier, inc=1, device_id={"pipe": 1 - section}, device_id_type=pl.DeviceIdType.MESH)
    pl.semaphore_wait(barrier, tensor + dp - 1)

    q_copies = over_tensor(qg.at[t], qg, "q")
    start(q_copies)
    q0_copy = remote(qg.at[t, pl.ds(0, rank)], q0, at("q0_s"), at("q0_r"), pipe=1 - section)
    gx_copy = remote(gqx, gqb.at[t], at("gx_s"), at("gx_r"), pipe=1 - section)
    piece = tokens // bulk

    def bulk_copy(i):
        rows = pl.ds(i * piece, piece)
        return remote(branch.at[rows], land.at[rows], at("bulk_s", i), at("bulk_r", i), pipe=1 - section)

    @pl.when(section == 0)
    def _():
        q0_copy.start()

    @pl.when(section == 1)
    def _():
        bulk_copy(0).start()
        gadd[...] = add_round(gtop[...], branch[...])
        gqb[t] = fold(mm(qg[t], gtop[...], NT)) * scale

    from_tensor(qg, "q")

    def eq_tile(i, carry):
        err_copy(i).wait()
        rows = pl.ds(pl.multiple_of(i * tile, tile), tile)
        total = mm(qg[0], err[rows, pl.ds(0, features)], NT)
        for tt in range(1, tensor):
            total += mm(qg[tt], err[rows, pl.ds(tt * features, features)], NT)
        eq[:, rows] = fold(total)
        return carry

    lax.fori_loop(0, tiles, eq_tile, 0)

    @pl.when(section == 1)
    def _():
        q0_copy.wait_recv()
        gqx[...] = mm(q0[...], gadd[...], NT) * scale
        gx_copy.start()
        for i in range(1, bulk):
            bulk_copy(i).start()

    @pl.when(section == 0)
    def _():
        gx_copy.wait_recv()

    gq_copies = over_tensor(gqb.at[t], gqb, "gq")
    start(gq_copies)
    from_tensor(gqb, "gq")
    gq = gqb[0]
    for tt in range(1, tensor):
        gq += gqb[tt]
    p_local = (fold(mm(terms(gq), attn[...], NN)) + eq[...]).astype(BF16)
    for j in range(dp):
        psend[j] = p_local[:, j * pw : (j + 1) * pw]
    p_copies = over_dp(lambda peer: psend.at[peer], prcv, "p")
    start(p_copies)
    from_dp(prcv, "p")
    total = psend[r].astype(F32)
    for peer in dp_peers:
        total += prcv[peer].astype(F32)
    pg[r] = (total * (1.0 / dp)).astype(BF16)
    pg_copies = over_dp(lambda peer: pg.at[r], pg, "pg")
    start(pg_copies)
    from_dp(pg, "pg")
    for j in range(dp):
        praw[:, j * pw : (j + 1) * pw] = pg[j]

    gb[t] = mm(praw[...], praw[...], NT)
    gram_copies = over_tensor(gb.at[t], gb, "gram")
    start(gram_copies)
    from_tensor(gb, "gram")
    gram = gb[0]
    for tt in range(1, tensor):
        gram += gb[tt]
    inverse = inverse_factor(gram)
    head = inverse.astype(BF16)
    rest = inverse - head.astype(F32)
    middle = rest.astype(BF16)
    last = (rest - middle.astype(F32)).astype(BF16)
    parts = mm(jnp.concatenate([head, middle, last], axis=0), praw[...], NN)
    p = parts[:rank] + (parts[rank : 2 * rank] + parts[2 * rank :])
    p_out[...] = p
    phl[...] = terms(p)
    apb[t] = fold(mm(phl[...], attn[...], NT)) * scale
    ap_copies = over_tensor(apb.at[t], apb, "ap")
    start(ap_copies)

    step = min(features, 512)

    def project(owner, done):
        def column(i, carry):
            here = pl.ds(pl.multiple_of(i * step, step), step)
            there = pl.ds(pl.multiple_of(owner * features + i * step, step), step)
            done(here, fold(mm(phl[...], err[:, there], NN)))
            return carry

        lax.fori_loop(0, features // step, column, 0)

    qx_copies = []
    for o, peer in enumerate(tensor_peers):
        def keep(here, value, slot=o):
            qx[slot, :, here] = value.astype(BF16)

        project(peer, keep)
        copy = remote(qx.at[o], qxr.at[t], at("qx_s", o), at("qx_r", t), tensor=peer)
        copy.start()
        qx_copies.append(copy)

    @pl.when(section == 0)
    def _():
        for i in range(bulk):
            bulk_copy(i).wait_recv()
        gbuf[t] = add_round(gtop[...], land[...])

    @pl.when(section == 1)
    def _():
        gbuf[t] = gtop[...]

    from_tensor(apb, "ap")
    ap = apb[0]
    for tt in range(1, tensor):
        ap += apb[tt]
    apt = terms(ap)

    def keep_own(here, value):
        eq[:, here] = value + fold(mm(apt, gbuf[t, :, here], NN))

    def own_column(i, carry):
        here = pl.ds(pl.multiple_of(i * step, step), step)
        there = pl.ds(pl.multiple_of(t * features + i * step, step), step)
        keep_own(here, fold(mm(phl[...], err[:, there], NN)))
        return carry

    lax.fori_loop(0, features // step, own_column, 0)
    from_tensor(qxr, "qx")
    q_local = eq[:, :features]
    for peer in tensor_peers:
        q_local += qxr[peer].astype(F32)
    q_local = q_local.astype(BF16)
    for j in range(dp):
        qsend[j] = q_local[:, j * qw : (j + 1) * qw]
    qp_copies = over_dp(lambda peer: qsend.at[peer], qrcv, "qp")
    start(qp_copies)
    g_copies = over_tensor(gbuf.at[t], gbuf, "g")
    start(g_copies)
    from_dp(qrcv, "qp")
    total = qsend[r].astype(F32)
    for peer in dp_peers:
        total += qrcv[peer].astype(F32)
    qf[t, r] = (total * (1.0 / dp)).astype(BF16)
    qg_copies = [
        remote(qf.at[t, r], qf.at[t, r], at("qg_s", o), at("qg_r", r), dp=peer)
        for o, peer in enumerate(dp_peers)
    ]
    start(qg_copies)
    qf_copies = []

    def forward(j):
        for o, peer in enumerate(tensor_peers):
            copy = remote(qf.at[t, j], qf.at[t, j], at("qf_s", o * dp + j), at("qf_r", t * dp + j), tensor=peer)
            copy.start()
            qf_copies.append(copy)

    forward(r)
    from_tensor(gbuf, "g")
    g_copy = pltpu.make_async_copy(gbuf, g_out, at("g_out"))
    g_copy.start()
    for peer in dp_peers:
        remote(qf.at[t, peer], qf.at[t, peer], at("qg_s"), at("qg_r", peer), dp=peer).wait_recv()
        forward(peer)
    for j in range(dp):
        q_own[:, j * qw : (j + 1) * qw] = qf[t, j].astype(F32)
    for peer in tensor_peers:
        for j in range(dp):
            remote(qf.at[peer, j], qf.at[peer, j], at("qf_s"), at("qf_r", peer * dp + j), tensor=peer).wait_recv()
    for tt in range(tensor):
        for j in range(dp):
            first = tt * features + j * qw
            q_out[:, first : first + qw] = qf[tt, j]

    @pl.when(section == 0)
    def _():
        q0_copy.wait_send()

    @pl.when(section == 1)
    def _():
        gx_copy.wait_send()
        for i in range(bulk):
            bulk_copy(i).wait_send()

    for copies in (q_copies, gq_copies, p_copies, pg_copies, gram_copies, ap_copies,
                   qx_copies, qp_copies, g_copies, qg_copies, qf_copies):
        sent(copies)
    g_copy.wait()


def chain(mesh, attn, gtop, branch, err, q_t):
    tensor, dp = mesh.shape["tensor"], mesh.shape["dp"]
    tokens, head_rows = attn.shape
    features = gtop.shape[1]
    rank = q_t.shape[0]
    tiles = max(1, head_rows // max(128, head_rows // 8))
    bulk = 8
    names, count = semaphore_map(tensor, dp, bulk, tiles)
    width = tensor * features
    pw, qw = head_rows // dp, features // dp
    wide = max(head_rows, features)
    vmem = pl.BlockSpec(memory_space=pltpu.VMEM)
    anywhere = pl.BlockSpec(memory_space=pl.ANY)
    return pl.pallas_call(
        functools.partial(chain_kernel, (tensor, dp, bulk, tiles, names)),
        out_shape=(
            jax.ShapeDtypeStruct((tensor, tokens, features), BF16),
            jax.ShapeDtypeStruct((rank, head_rows), F32),
            jax.ShapeDtypeStruct((rank, width), BF16),
            jax.ShapeDtypeStruct((rank, features), F32),
        ),
        in_specs=[vmem, vmem, vmem, anywhere, vmem],
        out_specs=(anywhere, vmem, vmem, vmem),
        scratch_shapes=[
            pltpu.VMEM((head_rows, width), BF16),
            pltpu.VMEM((tensor, 2 * rank, features), BF16),
            pltpu.VMEM((rank, features), BF16),
            pltpu.VMEM((tokens, features), BF16),
            pltpu.VMEM((tokens, features), BF16),
            pltpu.VMEM((tensor, tokens, features), BF16),
            pltpu.VMEM((rank, tokens), F32),
            pltpu.VMEM((tensor, rank, tokens), F32),
            pltpu.VMEM((rank, wide), F32),
            pltpu.VMEM((dp, rank, pw), BF16),
            pltpu.VMEM((dp, rank, pw), BF16),
            pltpu.VMEM((dp, rank, pw), BF16),
            pltpu.VMEM((rank, head_rows), BF16),
            pltpu.VMEM((tensor, rank, rank), F32),
            pltpu.VMEM((2 * rank, head_rows), BF16),
            pltpu.VMEM((tensor, rank, tokens), F32),
            pltpu.VMEM((max(1, tensor - 1), rank, features), BF16),
            pltpu.VMEM((tensor, rank, features), BF16),
            pltpu.VMEM((dp, rank, qw), BF16),
            pltpu.VMEM((dp, rank, qw), BF16),
            pltpu.VMEM((tensor, dp, rank, qw), BF16),
            pltpu.SemaphoreType.DMA((count,)),
        ],
        compiler_params=pltpu.CompilerParams(
            collective_id=0, has_side_effects=True, vmem_limit_bytes=56 * 2**20
        ),
        name="chain",
    )(attn, gtop, branch, err, q_t)


def error_kernel(attn, g, err, p, q, out, pair):
    tensor, tokens, features = g.shape
    scale = 1.0 / tokens

    @pl.when(pl.program_id(0) == 0)
    def _():
        pair[...] = jnp.concatenate([q[...], q[...]], axis=0)

    acts = attn[...].T
    fact = terms(p[...]).T
    step = min(features, 512)
    for tt in range(tensor):
        for c in range(features // step):
            here = slice(c * step, (c + 1) * step)
            there = slice(tt * features + c * step, tt * features + (c + 1) * step)
            matrix = mm(acts, g[tt, :, here], NN) * scale + err[:, there].astype(F32)
            out[:, there] = (matrix - mm(fact, pair[:, there], NN)).astype(BF16)


def error_next(attn, g, err, p, q):
    tensor, tokens, features = g.shape
    head_rows, width = err.shape
    rank = p.shape[0]
    tile = max(128, head_rows // 8)
    return pl.pallas_call(
        error_kernel,
        out_shape=jax.ShapeDtypeStruct((head_rows, width), BF16),
        grid=(head_rows // tile,),
        in_specs=[
            pl.BlockSpec((tokens, tile), lambda i: (0, i)),
            pl.BlockSpec((tensor, tokens, features), lambda i: (0, 0, 0)),
            pl.BlockSpec((tile, width), lambda i: (i, 0)),
            pl.BlockSpec((rank, tile), lambda i: (0, i)),
            pl.BlockSpec((rank, width), lambda i: (0, 0)),
        ],
        out_specs=pl.BlockSpec((tile, width), lambda i: (i, 0)),
        scratch_shapes=[pltpu.VMEM((2 * rank, width), BF16)],
        compiler_params=pltpu.CompilerParams(
            dimension_semantics=("arbitrary",), vmem_limit_bytes=48 * 2**20
        ),
        name="error_next",
    )(attn, g, err, p, q)


def on_device(mesh, attn_out, grad_top, branch_grad, error_prev, q_prev):
    micro, rows, features = grad_top.shape
    tokens = micro * rows
    attn = attn_out.reshape(tokens, attn_out.shape[3])
    gtop = grad_top.reshape(tokens, features)
    branch = branch_grad.reshape(tokens, features)
    err = error_prev[0, 0]
    g, p, q, q_own = chain(mesh, attn, gtop, branch, err, q_prev[0].T)
    own = lax.dynamic_index_in_dim(g, lax.axis_index("tensor"), 0, keepdims=False)
    grad_in = add_round(own, branch).reshape(branch_grad.shape)
    error = error_next(attn, g, err, p, q)
    return grad_in, error[None, None], p.T[None], q_own.T[None]


def solution(mesh):
    assert mesh.shape["pipe"] == 2
    return jax.shard_map(
        functools.partial(on_device, mesh),
        mesh=mesh,
        in_specs=(
            P("pipe", None, "dp", "tensor"),
            P(None, "dp", "tensor"),
            P("pipe", None, "dp", "tensor"),
            P("pipe", "dp", "tensor", None),
            P("pipe", "tensor", None),
        ),
        out_specs=(
            P("pipe", None, "dp", "tensor"),
            P("pipe", "dp", "tensor", None),
            P("pipe", "tensor", None),
            P("pipe", "tensor", None),
        ),
        check_vma=False,
    )
```

```python
import functools

import jax
import jax.numpy as jnp
from jax import lax
from jax.experimental import pallas as pl
from jax.experimental.pallas import tpu as pltpu
from jax.sharding import PartitionSpec as P

BF16 = jnp.bfloat16
F32 = jnp.float32
NN = (((1,), (0,)), ((), ()))
NT = (((1,), (1,)), ((), ()))
TN = (((0,), (0,)), ((), ()))


def mm(a, b, dims):
    return lax.dot_general(a, b, dims, preferred_element_type=F32)


def terms(x):
    head = x.astype(BF16)
    tail = (x - head.astype(F32)).astype(BF16)
    return jnp.concatenate([head, tail], axis=0)


def fold(y):
    half = y.shape[0] // 2
    return y[:half] + y[half:]


def add_round(a, b):
    return (a.astype(F32) + b.astype(F32)).astype(BF16)


def inverse_factor(gram):
    rank = gram.shape[0]
    row = lax.broadcasted_iota(jnp.int32, (rank, 2 * rank), 0)
    col = lax.broadcasted_iota(jnp.int32, (rank, 2 * rank), 1)
    work = jnp.concatenate([gram, jnp.where(row == col, 1.0, 0.0)[:, :rank]], axis=1)
    for k in range(rank - 1):
        ratio = work[:, k : k + 1] * (1.0 / work[k : k + 1, k : k + 1])
        work = work - jnp.where(row > k, ratio * work[k : k + 1, :], 0.0)
    diagonal = jnp.sum(jnp.where(row == col, work, 0.0), axis=1, keepdims=True)
    return work[:, rank:] * lax.rsqrt(diagonal)


class Semaphores:
    def __init__(self):
        self.count = 0

    def take(self, n=1):
        first = self.count
        self.count += n
        return first


def semaphore_map(tensor, dp, bulk, tiles):
    s = Semaphores()
    names = {}
    for name, n in (
        ("err", tiles),
        ("q_s", tensor), ("q_r", tensor), ("q0_s", 1), ("q0_r", 1),
        ("bulk_s", bulk), ("bulk_r", bulk), ("gx_s", 1), ("gx_r", 1),
        ("gq_s", tensor), ("gq_r", tensor), ("p_s", dp), ("p_r", dp),
        ("pg_s", dp), ("pg_r", dp), ("gram_s", tensor), ("gram_r", tensor),
        ("ap_s", tensor), ("ap_r", tensor), ("qx_s", tensor), ("qx_r", tensor),
        ("g_s", tensor * bulk), ("g_r", tensor * bulk), ("qp_s", dp), ("qp_r", dp),
        ("qg_s", dp), ("qg_r", dp), ("qf_s", tensor * dp), ("qf_r", tensor * dp),
    ):
        names[name] = s.take(n)
    return names, s.count


def chain_kernel(
    dims, attn, gtop, branch, err_hbm, q_in,
    err, grad_in, p_out, q_out, q_own,
    at_ref, qg, q0, land, gbuf, gqx, gqb, eq, psend, prcv, pg, praw, gb,
    phl, apb, qx, qxr, qsend, qrcv, qf, sem,
):
    tensor, dp, bulk, tiles, names = dims
    tokens, head_rows = attn.shape
    features = gtop.shape[1]
    rank = q_in.shape[0]
    pw, qw = head_rows // dp, features // dp
    section = lax.axis_index("pipe")
    t = lax.axis_index("tensor")
    r = lax.axis_index("dp")
    scale = 1.0 / tokens

    def at(name, index=0):
        return sem.at[names[name] + index]

    def remote(src, dst, send, recv, **where):
        return pltpu.make_async_remote_copy(
            src_ref=src, dst_ref=dst, send_sem=send, recv_sem=recv,
            device_id=where, device_id_type=pl.DeviceIdType.MESH,
        )

    tensor_peers = [lax.rem(t + o, tensor) for o in range(1, tensor)]
    dp_peers = [lax.rem(r + o, dp) for o in range(1, dp)]

    def over_tensor(src, dst, key):
        return [
            remote(src, dst.at[t], at(key + "_s", o), at(key + "_r", t), tensor=peer)
            for o, peer in enumerate(tensor_peers)
        ]

    def from_tensor(dst, key):
        for peer in tensor_peers:
            remote(dst.at[peer], dst.at[peer], at(key + "_s"), at(key + "_r", peer), tensor=peer).wait_recv()

    def over_dp(src_of, dst, key):
        return [
            remote(src_of(peer), dst.at[r], at(key + "_s", o), at(key + "_r", r), dp=peer)
            for o, peer in enumerate(dp_peers)
        ]

    def from_dp(dst, key):
        for peer in dp_peers:
            remote(dst.at[peer], dst.at[peer], at(key + "_s"), at(key + "_r", peer), dp=peer).wait_recv()

    def start(copies):
        for copy in copies:
            copy.start()

    def sent(copies):
        for copy in copies:
            copy.wait_send()

    tile = head_rows // tiles

    def err_copy(i):
        rows = pl.ds(pl.multiple_of(i * tile, tile), tile)
        return pltpu.make_async_copy(err_hbm.at[rows], err.at[rows], at("err", i))

    for i in range(tiles):
        err_copy(i).start()
    qg[t] = terms(q_in[...])

    barrier = pltpu.get_barrier_semaphore()
    for peer in tensor_peers:
        pl.semaphore_signal(barrier, inc=1, device_id={"tensor": peer}, device_id_type=pl.DeviceIdType.MESH)
    for peer in dp_peers:
        pl.semaphore_signal(barrier, inc=1, device_id={"dp": peer}, device_id_type=pl.DeviceIdType.MESH)
    pl.semaphore_signal(barrier, inc=1, device_id={"pipe": 1 - section}, device_id_type=pl.DeviceIdType.MESH)
    pl.semaphore_wait(barrier, tensor + dp - 1)

    q_copies = over_tensor(qg.at[t], qg, "q")
    start(q_copies)
    q0_copy = remote(qg.at[t, pl.ds(0, rank)], q0, at("q0_s"), at("q0_r"), pipe=1 - section)
    gx_copy = remote(gqx, gqb.at[t], at("gx_s"), at("gx_r"), pipe=1 - section)
    piece = tokens // bulk
    ahead = bulk // 4

    def bulk_copy(i):
        rows = pl.ds(pl.multiple_of(i * piece, piece), piece)
        return remote(branch.at[rows], land.at[rows], at("bulk_s", i), at("bulk_r", i), pipe=1 - section)

    @pl.when(section == 0)
    def _():
        q0_copy.start()

    @pl.when(section == 1)
    def _():
        for i in range(ahead):
            bulk_copy(i).start()
        grad_in[...] = add_round(gtop[...], branch[...])
        gqb[t] = fold(mm(qg[t], gtop[...], NT)) * scale

    from_tensor(qg, "q")

    def eq_tile(i, carry):
        err_copy(i).wait()
        rows = pl.ds(pl.multiple_of(i * tile, tile), tile)
        total = mm(qg[0], err[rows, pl.ds(0, features)], NT)
        for tt in range(1, tensor):
            total += mm(qg[tt], err[rows, pl.ds(tt * features, features)], NT)
        eq[:, rows] = fold(total)
        return carry

    lax.fori_loop(0, tiles, eq_tile, 0)

    @pl.when(section == 1)
    def _():
        q0_copy.wait_recv()
        gqx[...] = mm(q0[...], grad_in[...], NT) * scale
        gx_copy.start()
        for i in range(ahead, bulk):
            bulk_copy(i).start()

    @pl.when(section == 0)
    def _():
        gx_copy.wait_recv()

    gq_copies = over_tensor(gqb.at[t], gqb, "gq")
    start(gq_copies)
    from_tensor(gqb, "gq")
    gq = gqb[0]
    for tt in range(1, tensor):
        gq += gqb[tt]
    p_local = (fold(mm(terms(gq), attn[...], NN)) + eq[...]).astype(BF16)
    for j in range(dp):
        psend[j] = p_local[:, j * pw : (j + 1) * pw]
    p_copies = over_dp(lambda peer: psend.at[peer], prcv, "p")
    start(p_copies)

    def transpose_tile(i, carry):
        rows = pl.ds(pl.multiple_of(i * tile, tile), tile)
        at_ref[rows, :] = attn[:, rows].T
        return carry

    lax.fori_loop(0, tiles, transpose_tile, 0)
    from_dp(prcv, "p")
    total = psend[r].astype(F32)
    for peer in dp_peers:
        total += prcv[peer].astype(F32)
    pg[r] = (total * (1.0 / dp)).astype(BF16)
    pg_copies = over_dp(lambda peer: pg.at[r], pg, "pg")
    start(pg_copies)
    from_dp(pg, "pg")
    for j in range(dp):
        praw[:, j * pw : (j + 1) * pw] = pg[j]

    gb[t] = mm(praw[...], praw[...], NT)
    gram_copies = over_tensor(gb.at[t], gb, "gram")
    start(gram_copies)
    from_tensor(gb, "gram")
    gram = gb[0]
    for tt in range(1, tensor):
        gram += gb[tt]
    inverse = inverse_factor(gram)
    head = inverse.astype(BF16)
    rest = inverse - head.astype(F32)
    middle = rest.astype(BF16)
    last = (rest - middle.astype(F32)).astype(BF16)
    parts = mm(jnp.concatenate([head, middle, last], axis=0), praw[...], NN)
    p = parts[:rank] + (parts[rank : 2 * rank] + parts[2 * rank :])
    p_out[...] = p
    phl[...] = terms(p)
    apb[t] = fold(mm(phl[...], attn[...], NT)) * scale
    ap_copies = over_tensor(apb.at[t], apb, "ap")
    start(ap_copies)

    step = min(features, 512)

    def project(owner, done):
        def column(i, carry):
            here = pl.ds(pl.multiple_of(i * step, step), step)
            there = pl.ds(pl.multiple_of(owner * features + i * step, step), step)
            done(here, fold(mm(phl[...], err[:, there], NN)))
            return carry

        lax.fori_loop(0, features // step, column, 0)

    qx_copies = []
    for o, peer in enumerate(tensor_peers):
        def keep(here, value, slot=o):
            qx[slot, :, here] = value.astype(BF16)

        project(peer, keep)
        copy = remote(qx.at[o], qxr.at[t], at("qx_s", o), at("qx_r", t), tensor=peer)
        copy.start()
        qx_copies.append(copy)

    def g_copies(i):
        rows = pl.ds(pl.multiple_of(i * piece, piece), piece)
        return [
            remote(gbuf.at[t, rows], gbuf.at[t, rows], at("g_s", o * bulk + i), at("g_r", t * bulk + i), tensor=peer)
            for o, peer in enumerate(tensor_peers)
        ]

    def land_piece(i, carry):
        rows = pl.ds(pl.multiple_of(i * piece, piece), piece)

        @pl.when(section == 0)
        def _():
            bulk_copy(i).wait_recv()
            out_grad = add_round(gtop[rows, :], land[rows, :])
            gbuf[t, rows, :] = out_grad
            grad_in[rows, :] = add_round(out_grad, branch[rows, :])

        @pl.when(section == 1)
        def _():
            gbuf[t, rows, :] = gtop[rows, :]

        start(g_copies(i))
        return carry

    lax.fori_loop(0, bulk, land_piece, 0)

    from_tensor(apb, "ap")
    ap = apb[0]
    for tt in range(1, tensor):
        ap += apb[tt]
    apt = terms(ap)

    def keep_own(here, value):
        eq[:, here] = value + fold(mm(apt, gbuf[t, :, here], NN))

    def own_column(i, carry):
        here = pl.ds(pl.multiple_of(i * step, step), step)
        there = pl.ds(pl.multiple_of(t * features + i * step, step), step)
        keep_own(here, fold(mm(phl[...], err[:, there], NN)))
        return carry

    lax.fori_loop(0, features // step, own_column, 0)
    from_tensor(qxr, "qx")
    q_local = eq[:, :features]
    for peer in tensor_peers:
        q_local += qxr[peer].astype(F32)
    q_local = q_local.astype(BF16)
    for j in range(dp):
        qsend[j] = q_local[:, j * qw : (j + 1) * qw]
    qp_copies = over_dp(lambda peer: qsend.at[peer], qrcv, "qp")
    start(qp_copies)

    def g_landed(i, carry):
        rows = pl.ds(pl.multiple_of(i * piece, piece), piece)
        for peer in tensor_peers:
            here = gbuf.at[peer, rows]
            remote(here, here, at("g_s"), at("g_r", peer * bulk + i), tensor=peer).wait_recv()
        return carry

    lax.fori_loop(0, bulk, g_landed, 0)

    def matrix_tile(i, carry):
        rows = pl.ds(pl.multiple_of(i * tile, tile), tile)
        acts = at_ref[rows, :]
        for tt in range(tensor):
            for c in range(features // step):
                here = pl.ds(c * step, step)
                there = pl.ds(tt * features + c * step, step)
                value = mm(acts, gbuf[tt, :, here], NN) * scale + err[rows, there].astype(F32)
                err[rows, there] = value.astype(BF16)
        return carry

    lax.fori_loop(0, tiles // 2, matrix_tile, 0)
    from_dp(qrcv, "qp")
    total = qsend[r].astype(F32)
    for peer in dp_peers:
        total += qrcv[peer].astype(F32)
    qf[t, r] = (total * (1.0 / dp)).astype(BF16)
    qg_copies = [
        remote(qf.at[t, r], qf.at[t, r], at("qg_s", o), at("qg_r", r), dp=peer)
        for o, peer in enumerate(dp_peers)
    ]
    start(qg_copies)
    qf_copies = []

    def forward(j):
        for o, peer in enumerate(tensor_peers):
            copy = remote(qf.at[t, j], qf.at[t, j], at("qf_s", o * dp + j), at("qf_r", t * dp + j), tensor=peer)
            copy.start()
            qf_copies.append(copy)

    forward(r)
    lax.fori_loop(tiles // 2, tiles, matrix_tile, 0)
    for peer in dp_peers:
        remote(qf.at[t, peer], qf.at[t, peer], at("qg_s"), at("qg_r", peer), dp=peer).wait_recv()
        forward(peer)
    for j in range(dp):
        q_own[:, j * qw : (j + 1) * qw] = qf[t, j].astype(F32)
    for peer in tensor_peers:
        for j in range(dp):
            remote(qf.at[peer, j], qf.at[peer, j], at("qf_s"), at("qf_r", peer * dp + j), tensor=peer).wait_recv()
    for tt in range(tensor):
        for j in range(dp):
            first = tt * features + j * qw
            q_out[:, first : first + qw] = qf[tt, j]

    @pl.when(section == 0)
    def _():
        q0_copy.wait_send()

    @pl.when(section == 1)
    def _():
        gx_copy.wait_send()
        for i in range(bulk):
            bulk_copy(i).wait_send()

    for copies in (q_copies, gq_copies, p_copies, pg_copies, gram_copies, ap_copies,
                   qx_copies, qp_copies, qg_copies, qf_copies):
        sent(copies)

    def g_sent(i, carry):
        sent(g_copies(i))
        return carry

    lax.fori_loop(0, bulk, g_sent, 0)


def chain(mesh, attn, gtop, branch, err, q_t):
    tensor, dp = mesh.shape["tensor"], mesh.shape["dp"]
    tokens, head_rows = attn.shape
    features = gtop.shape[1]
    rank = q_t.shape[0]
    tiles = max(1, head_rows // max(128, head_rows // 8))
    bulk = 16
    names, count = semaphore_map(tensor, dp, bulk, tiles)
    width = tensor * features
    pw, qw = head_rows // dp, features // dp
    wide = max(head_rows, features)
    vmem = pl.BlockSpec(memory_space=pltpu.VMEM)
    anywhere = pl.BlockSpec(memory_space=pl.ANY)
    return pl.pallas_call(
        functools.partial(chain_kernel, (tensor, dp, bulk, tiles, names)),
        out_shape=(
            pltpu.VMEM((head_rows, width), BF16),
            pltpu.VMEM((tokens, features), BF16),
            pltpu.VMEM((rank, head_rows), F32),
            pltpu.VMEM((rank, width), BF16),
            pltpu.VMEM((rank, features), F32),
        ),
        in_specs=[vmem, vmem, vmem, anywhere, vmem],
        out_specs=(vmem,) * 5,
        scratch_shapes=[
            pltpu.VMEM((head_rows, tokens), BF16),
            pltpu.VMEM((tensor, 2 * rank, features), BF16),
            pltpu.VMEM((rank, features), BF16),
            pltpu.VMEM((tokens, features), BF16),
            pltpu.VMEM((tensor, tokens, features), BF16),
            pltpu.VMEM((rank, tokens), F32),
            pltpu.VMEM((tensor, rank, tokens), F32),
            pltpu.VMEM((rank, wide), F32),
            pltpu.VMEM((dp, rank, pw), BF16),
            pltpu.VMEM((dp, rank, pw), BF16),
            pltpu.VMEM((dp, rank, pw), BF16),
            pltpu.VMEM((rank, head_rows), BF16),
            pltpu.VMEM((tensor, rank, rank), F32),
            pltpu.VMEM((2 * rank, head_rows), BF16),
            pltpu.VMEM((tensor, rank, tokens), F32),
            pltpu.VMEM((max(1, tensor - 1), rank, features), BF16),
            pltpu.VMEM((tensor, rank, features), BF16),
            pltpu.VMEM((dp, rank, qw), BF16),
            pltpu.VMEM((dp, rank, qw), BF16),
            pltpu.VMEM((tensor, dp, rank, qw), BF16),
            pltpu.SemaphoreType.DMA((count,)),
        ],
        compiler_params=pltpu.CompilerParams(
            collective_id=0, has_side_effects=True, vmem_limit_bytes=30 * 2**20
        ),
        name="chain",
    )(attn, gtop, branch, err, q_t)


def finish_kernel(tiles, matrix, grad_in, p, q, q_own, out, grad_out, p_out, q_out, fact, pair, held, sem):
    head_rows, width = matrix.shape
    tile = head_rows // tiles
    step = min(width, 512)
    small = [
        pltpu.make_async_copy(src, dst, sem.at[2 + i])
        for i, (src, dst) in enumerate(((grad_in, grad_out), (p, p_out), (q_own, q_out)))
    ]
    for copy in small:
        copy.start()
    pair[...] = jnp.concatenate([q[...], q[...]], axis=0)
    fact[...] = terms(p[...]).T

    def out_copy(i, slot):
        rows = pl.ds(pl.multiple_of(i * tile, tile), tile)
        return pltpu.make_async_copy(held.at[slot], out.at[rows], sem.at[slot])

    def row_tile(i, carry):
        slot = lax.rem(i, 2)
        rows = pl.ds(pl.multiple_of(i * tile, tile), tile)

        @pl.when(i >= 2)
        def _():
            out_copy(i - 2, slot).wait()

        for c in range(width // step):
            here = slice(c * step, (c + 1) * step)
            value = matrix[rows, here].astype(F32) - mm(fact[rows, :], pair[:, here], NN)
            held[slot, :, here] = value.astype(BF16)
        out_copy(i, slot).start()
        return carry

    lax.fori_loop(0, tiles, row_tile, 0)
    for i in range(max(0, tiles - 2), tiles):
        out_copy(i, i % 2).wait()
    for copy in small:
        copy.wait()


def finish(matrix, grad_in, p, q, q_own):
    head_rows, width = matrix.shape
    rank = p.shape[0]
    tile = max(128, head_rows // 16)
    vmem = pl.BlockSpec(memory_space=pltpu.VMEM)
    anywhere = pl.BlockSpec(memory_space=pl.ANY)
    args = [pltpu.with_memory_space_constraint(x, pltpu.VMEM) for x in (matrix, grad_in, p, q, q_own)]
    return pl.pallas_call(
        functools.partial(finish_kernel, head_rows // tile),
        out_shape=(
            pltpu.HBM(matrix.shape, BF16),
            pltpu.HBM(grad_in.shape, BF16),
            pltpu.HBM(p.shape, F32),
            pltpu.HBM(q_own.shape, F32),
        ),
        in_specs=[vmem] * 5,
        out_specs=(anywhere,) * 4,
        scratch_shapes=[
            pltpu.VMEM((head_rows, 2 * rank), BF16),
            pltpu.VMEM((2 * rank, width), BF16),
            pltpu.VMEM((2, tile, width), BF16),
            pltpu.SemaphoreType.DMA((5,)),
        ],
        compiler_params=pltpu.CompilerParams(vmem_limit_bytes=12 * 2**20),
        name="finish",
    )(*args)


def on_device(mesh, attn_out, grad_top, branch_grad, error_prev, q_prev):
    micro, rows, features = grad_top.shape
    tokens = micro * rows
    attn = attn_out.reshape(tokens, attn_out.shape[3])
    gtop = grad_top.reshape(tokens, features)
    branch = branch_grad.reshape(tokens, features)
    err = error_prev[0, 0]
    matrix, grad_in, p, q, q_own = chain(mesh, attn, gtop, branch, err, q_prev[0].T)
    error, grad_in, p, q_own = finish(matrix, grad_in, p, q, q_own)
    return grad_in.reshape(branch_grad.shape), error[None, None], p.T[None], q_own.T[None]


def solution(mesh):
    assert mesh.shape["pipe"] == 2
    return jax.shard_map(
        functools.partial(on_device, mesh),
        mesh=mesh,
        in_specs=(
            P("pipe", None, "dp", "tensor"),
            P(None, "dp", "tensor"),
            P("pipe", None, "dp", "tensor"),
            P("pipe", "dp", "tensor", None),
            P("pipe", "tensor", None),
        ),
        out_specs=(
            P("pipe", None, "dp", "tensor"),
            P("pipe", "dp", "tensor", None),
            P("pipe", "tensor", None),
            P("pipe", "tensor", None),
        ),
        check_vma=False,
    )
```

```python
import functools

import jax
import jax.numpy as jnp
from jax import lax
from jax.experimental import pallas as pl
from jax.experimental.pallas import tpu as pltpu
from jax.sharding import PartitionSpec as P

BF16 = jnp.bfloat16
F32 = jnp.float32
NN = (((1,), (0,)), ((), ()))
NT = (((1,), (1,)), ((), ()))
TN = (((0,), (0,)), ((), ()))


def mm(a, b, dims):
    return lax.dot_general(a, b, dims, preferred_element_type=F32)


def terms(x):
    head = x.astype(BF16)
    tail = (x - head.astype(F32)).astype(BF16)
    return jnp.concatenate([head, tail], axis=0)


def fold(y):
    half = y.shape[0] // 2
    return y[:half] + y[half:]


def add_round(a, b):
    return (a.astype(F32) + b.astype(F32)).astype(BF16)


def inverse_factor(gram):
    rank = gram.shape[0]
    row = lax.broadcasted_iota(jnp.int32, (rank, 2 * rank), 0)
    col = lax.broadcasted_iota(jnp.int32, (rank, 2 * rank), 1)
    work = jnp.concatenate([gram, jnp.where(row == col, 1.0, 0.0)[:, :rank]], axis=1)
    for k in range(rank - 1):
        ratio = work[:, k : k + 1] * (1.0 / work[k : k + 1, k : k + 1])
        work = work - jnp.where(row > k, ratio * work[k : k + 1, :], 0.0)
    diagonal = jnp.sum(jnp.where(row == col, work, 0.0), axis=1, keepdims=True)
    return work[:, rank:] * lax.rsqrt(diagonal)


class Semaphores:
    def __init__(self):
        self.count = 0

    def take(self, n=1):
        first = self.count
        self.count += n
        return first


def semaphore_map(tensor, dp, units, tiles):
    s = Semaphores()
    names = {}
    for name, n in (
        ("err", tiles), ("load", 4),
        ("q_s", tensor), ("q_r", tensor), ("q0_s", 1), ("q0_r", 1),
        ("bulk_s", units), ("bulk_r", units), ("gx_s", 1), ("gx_r", 1),
        ("gq_s", tensor), ("gq_r", tensor), ("p_s", dp), ("p_r", dp),
        ("pg_s", dp), ("pg_r", dp), ("gram_s", tensor), ("gram_r", tensor),
        ("ap_s", tensor), ("ap_r", tensor), ("qx_s", tensor), ("qx_r", tensor),
        ("g_s", tensor * units), ("g_r", tensor * units), ("qp_s", dp), ("qp_r", dp),
        ("qg_s", dp), ("qg_r", dp), ("qf_s", tensor * dp), ("qf_r", tensor * dp),
    ):
        names[name] = s.take(n)
    return names, s.count


def chain_kernel(
    dims, attn_hbm, gtop_hbm, branch_hbm, err_hbm, q_hbm,
    matrix, grad_in, p_out, fact, pair, q_own,
    attn, gtop, branch, err, q_in, at_ref, qg, q0, gbuf, gqx, gqr, gqb, eq,
    psend, prcv, pg, praw, gb, lin, apb, apt, qx, qxr, qsend, qrcv, qf, sem,
):
    tensor, dp, units, tiles, names = dims
    tokens, head_rows = attn.shape
    features = gtop.shape[1]
    rank = q_in.shape[0]
    pw, qw = head_rows // dp, features // dp
    unit = features // units
    shards = unit // qw
    section = lax.axis_index("pipe")
    t = lax.axis_index("tensor")
    r = lax.axis_index("dp")
    scale = 1.0 / tokens

    def at(name, index=0):
        return sem.at[names[name] + index]

    def remote(src, dst, send, recv, **where):
        return pltpu.make_async_remote_copy(
            src_ref=src, dst_ref=dst, send_sem=send, recv_sem=recv,
            device_id=where, device_id_type=pl.DeviceIdType.MESH,
        )

    tensor_peers = [lax.rem(t + o, tensor) for o in range(1, tensor)]
    dp_peers = [lax.rem(r + o, dp) for o in range(1, dp)]

    def over_tensor(src, dst, key):
        return [
            remote(src, dst.at[t], at(key + "_s", o), at(key + "_r", t), tensor=peer)
            for o, peer in enumerate(tensor_peers)
        ]

    def from_tensor(dst, key):
        for peer in tensor_peers:
            remote(dst.at[peer], dst.at[peer], at(key + "_s"), at(key + "_r", peer), tensor=peer).wait_recv()

    def over_dp(src_of, dst, key):
        return [
            remote(src_of(peer), dst.at[r], at(key + "_s", o), at(key + "_r", r), dp=peer)
            for o, peer in enumerate(dp_peers)
        ]

    def from_dp(dst, key):
        for peer in dp_peers:
            remote(dst.at[peer], dst.at[peer], at(key + "_s"), at(key + "_r", peer), dp=peer).wait_recv()

    def start(copies):
        for copy in copies:
            copy.start()

    def sent(copies):
        for copy in copies:
            copy.wait_send()

    def columns(i):
        return pl.ds(pl.multiple_of(i * unit, unit), unit)

    tile = head_rows // tiles

    def err_copy(i):
        rows = pl.ds(pl.multiple_of(i * tile, tile), tile)
        return pltpu.make_async_copy(err_hbm.at[rows], err.at[rows], at("err", i))

    loads = [
        pltpu.make_async_copy(src, dst, at("load", i))
        for i, (src, dst) in enumerate(
            ((q_hbm, q_in), (branch_hbm, branch), (gtop_hbm, gtop), (attn_hbm, attn))
        )
    ]
    start(loads)
    for i in range(tiles):
        err_copy(i).start()

    barrier = pltpu.get_barrier_semaphore()
    for peer in tensor_peers:
        pl.semaphore_signal(barrier, inc=1, device_id={"tensor": peer}, device_id_type=pl.DeviceIdType.MESH)
    for peer in dp_peers:
        pl.semaphore_signal(barrier, inc=1, device_id={"dp": peer}, device_id_type=pl.DeviceIdType.MESH)
    pl.semaphore_signal(barrier, inc=1, device_id={"pipe": 1 - section}, device_id_type=pl.DeviceIdType.MESH)
    loads[0].wait()
    qg[t] = terms(q_in[...])
    loads[1].wait()
    pl.semaphore_wait(barrier, tensor + dp - 1)

    q0_copy = remote(qg.at[t, pl.ds(0, rank)], q0, at("q0_s"), at("q0_r"), pipe=1 - section)
    gx_copy = remote(gqx, gqr, at("gx_s"), at("gx_r"), pipe=1 - section)
    ahead = units // 4

    def bulk_copy(i):
        return remote(branch.at[:, columns(i)], gbuf.at[t, :, columns(i)], at("bulk_s", i), at("bulk_r", i), pipe=1 - section)

    @pl.when(section == 0)
    def _():
        q0_copy.start()

    @pl.when(section == 1)
    def _():
        for i in range(ahead):
            bulk_copy(i).start()

    q_copies = over_tensor(qg.at[t], qg, "q")
    start(q_copies)
    loads[2].wait()
    loads[3].wait()

    @pl.when(section == 1)
    def _():
        grad_in[...] = add_round(gtop[...], branch[...])
        gqb[t] = fold(mm(qg[t], gtop[...], NT)) * scale

    from_tensor(qg, "q")

    def eq_tile(i, carry):
        err_copy(i).wait()
        rows = pl.ds(pl.multiple_of(i * tile, tile), tile)
        total = mm(qg[0], err[rows, pl.ds(0, features)], NT)
        for tt in range(1, tensor):
            total += mm(qg[tt], err[rows, pl.ds(tt * features, features)], NT)
        eq[:, rows] = fold(total)
        return carry

    lax.fori_loop(0, tiles, eq_tile, 0)

    @pl.when(section == 1)
    def _():
        q0_copy.wait_recv()
        gqx[...] = (mm(q0[...], grad_in[...], NT) * scale).astype(BF16)
        gx_copy.start()
        for i in range(ahead, units):
            bulk_copy(i).start()

    @pl.when(section == 0)
    def _():
        gx_copy.wait_recv()
        gqb[t] = gqr[...].astype(F32)

    gq_copies = over_tensor(gqb.at[t], gqb, "gq")
    start(gq_copies)
    from_tensor(gqb, "gq")
    gq = gqb[0]
    for tt in range(1, tensor):
        gq += gqb[tt]
    p_local = (fold(mm(terms(gq), attn[...], NN)) + eq[:, :head_rows]).astype(BF16)
    for j in range(dp):
        psend[j] = p_local[:, j * pw : (j + 1) * pw]
    p_copies = over_dp(lambda peer: psend.at[peer], prcv, "p")
    start(p_copies)

    def g_copies(i):
        here = gbuf.at[t, :, columns(i)]
        return [
            remote(here, here, at("g_s", o * units + i), at("g_r", t * units + i), tensor=peer)
            for o, peer in enumerate(tensor_peers)
        ]

    def land_unit(i, carry):
        cols = columns(i)

        @pl.when(section == 0)
        def _():
            bulk_copy(i).wait_recv()
            out_grad = add_round(gtop[:, cols], gbuf[t, :, cols])
            gbuf[t, :, cols] = out_grad
            grad_in[:, cols] = add_round(out_grad, branch[:, cols])

        @pl.when(section == 1)
        def _():
            gbuf[t, :, cols] = gtop[:, cols]

        start(g_copies(i))
        return carry

    def matrix_unit(i, carry):
        cols = columns(i)
        for peer in tensor_peers:
            here = gbuf.at[peer, :, cols]
            remote(here, here, at("g_s"), at("g_r", peer * units + i), tensor=peer).wait_recv()
        block = min(head_rows, 512)
        for tt in range(tensor):
            there = pl.ds(pl.multiple_of(tt * features + i * unit, unit), unit)
            grads = gbuf[tt, :, cols]
            for c in range(head_rows // block):
                rows = pl.ds(c * block, block)
                value = mm(at_ref[rows, :], grads, NN) * scale + err[rows, there].astype(F32)
                matrix[rows, there] = value.astype(BF16)
        return carry

    def transpose_tile(i, carry):
        rows = pl.ds(pl.multiple_of(i * tile, tile), tile)
        at_ref[rows, :] = attn[:, rows].T
        return carry

    first, second, third = units // 4, 3 * units // 8, 5 * units // 8
    lax.fori_loop(0, tiles, transpose_tile, 0)
    lax.fori_loop(0, first, land_unit, 0)
    lax.fori_loop(0, first, matrix_unit, 0)
    from_dp(prcv, "p")
    total = psend[r].astype(F32)
    for peer in dp_peers:
        total += prcv[peer].astype(F32)
    pg[r] = (total * (1.0 / dp)).astype(BF16)
    pg_copies = over_dp(lambda peer: pg.at[r], pg, "pg")
    start(pg_copies)
    lax.fori_loop(first, second, land_unit, 0)
    lax.fori_loop(first, second, matrix_unit, 0)
    from_dp(pg, "pg")
    for j in range(dp):
        praw[:, j * pw : (j + 1) * pw] = pg[j]

    gb[t] = mm(praw[...], praw[...], NT)
    gram_copies = over_tensor(gb.at[t], gb, "gram")
    start(gram_copies)
    apb[t] = mm(praw[...], attn[...], NT) * scale
    ap_copies = over_tensor(apb.at[t], apb, "ap")
    start(ap_copies)

    step = min(features, 512)

    def project(owner, done):
        def column(i, carry):
            here = pl.ds(pl.multiple_of(i * step, step), step)
            there = pl.ds(pl.multiple_of(owner * features + i * step, step), step)
            done(here, mm(praw[...], err[:, there], NN))
            return carry

        lax.fori_loop(0, features // step, column, 0)

    qx_copies = []
    for o, peer in enumerate(tensor_peers):
        def keep(here, value, slot=o):
            qx[slot, :, here] = value.astype(BF16)

        project(peer, keep)
        copy = remote(qx.at[o], qxr.at[t], at("qx_s", o), at("qx_r", t), tensor=peer)
        copy.start()
        qx_copies.append(copy)

    def keep_own(here, value):
        eq[:, here] = value

    project(t, keep_own)
    lax.fori_loop(second, third, land_unit, 0)
    from_tensor(apb, "ap")
    ap = apb[0]
    for tt in range(1, tensor):
        ap += apb[tt]
    apt[...] = terms(ap)
    from_tensor(qxr, "qx")

    def q_copy(j):
        return remote(qsend.at[j], qrcv.at[r], at("qp_s", j), at("qp_r", r), dp=j)

    def q_unit(i, carry):
        cols = columns(i)
        value = eq[:, cols] + fold(mm(apt[...], gbuf[t, :, cols], NN))
        for peer in tensor_peers:
            value += qxr[peer, :, cols].astype(F32)
        value = value.astype(BF16)
        for k in range(shards):
            j = i * shards + k
            qsend[j] = value[:, k * qw : (k + 1) * qw]

            @pl.when(j != r)
            def _():
                q_copy(j).start()

        return carry

    def qg_copies():
        return [
            remote(qf.at[t, r], qf.at[t, r], at("qg_s", o), at("qg_r", r), dp=peer)
            for o, peer in enumerate(dp_peers)
        ]

    def forward(j):
        return [
            remote(qf.at[t, j], qf.at[t, j], at("qf_s", o * dp + j), at("qf_r", t * dp + j), tensor=peer)
            for o, peer in enumerate(tensor_peers)
        ]

    def reduce_q():
        from_dp(qrcv, "qp")
        total = qsend[r].astype(F32)
        for peer in dp_peers:
            total += qrcv[peer].astype(F32)
        qf[t, r] = (total * (1.0 / dp)).astype(BF16)
        start(qg_copies())
        start(forward(r))

    lax.fori_loop(0, third, q_unit, 0)

    from_tensor(gb, "gram")
    gram = gb[0]
    for tt in range(1, tensor):
        gram += gb[tt]
    inverse = inverse_factor(gram)
    head = inverse.astype(BF16)
    rest = inverse - head.astype(F32)
    middle = rest.astype(BF16)
    last = (rest - middle.astype(F32)).astype(BF16)
    lin[...] = jnp.concatenate([head, middle, last], axis=0)

    def applied(rows):
        parts = mm(lin[...], rows, NN)
        return parts[:rank] + (parts[rank : 2 * rank] + parts[2 * rank :])


    def late_unit(i, carry):
        land_unit(i, 0)
        return q_unit(i, carry)

    lax.fori_loop(third, units - 1, late_unit, 0)
    p = applied(praw[...])
    p_out[...] = p
    fact[...] = terms(p).T
    middle_unit = min(units - 1, second + 2)
    lax.fori_loop(second, middle_unit, matrix_unit, 0)

    @pl.when(r < dp - shards)
    def _():
        reduce_q()

    late_unit(units - 1, 0)
    later_unit = min(units, middle_unit + 2)
    lax.fori_loop(middle_unit, later_unit, matrix_unit, 0)

    @pl.when(r >= dp - shards)
    def _():
        reduce_q()

    lax.fori_loop(later_unit, units, matrix_unit, 0)

    def gather_q(j, carry):
        @pl.when(j != r)
        def _():
            remote(qf.at[t, j], qf.at[t, j], at("qg_s"), at("qg_r", j), dp=j).wait_recv()
            start(forward(j))

        return carry

    lax.fori_loop(0, dp, gather_q, 0)
    for j in range(dp):
        q_own[:, j * qw : (j + 1) * qw] = applied(qf[t, j])
    for peer in tensor_peers:
        for j in range(dp):
            remote(qf.at[peer, j], qf.at[peer, j], at("qf_s"), at("qf_r", peer * dp + j), tensor=peer).wait_recv()
    for tt in range(tensor):
        for j in range(dp):
            begin = tt * features + j * qw
            value = applied(qf[tt, j]).astype(BF16)
            pair[:rank, begin : begin + qw] = value
            pair[rank:, begin : begin + qw] = value

    @pl.when(section == 0)
    def _():
        q0_copy.wait_send()

    @pl.when(section == 1)
    def _():
        gx_copy.wait_send()
        for i in range(units):
            bulk_copy(i).wait_send()

    for copies in (q_copies, gq_copies, p_copies, pg_copies, gram_copies, ap_copies,
                   qx_copies, qg_copies()):
        sent(copies)

    def rows_sent(j, carry):
        sent(forward(j))

        @pl.when(j != r)
        def _():
            q_copy(j).wait_send()

        return carry

    lax.fori_loop(0, dp, rows_sent, 0)

    def g_sent(i, carry):
        sent(g_copies(i))
        return carry

    lax.fori_loop(0, units, g_sent, 0)


def chain(mesh, attn, gtop, branch, err, q_t):
    tensor, dp = mesh.shape["tensor"], mesh.shape["dp"]
    tokens, head_rows = attn.shape
    features = gtop.shape[1]
    rank = q_t.shape[0]
    tiles = max(1, head_rows // max(128, head_rows // 8))
    width = tensor * features
    pw, qw = head_rows // dp, features // dp
    units = features // max(128, features // 8, qw)
    names, count = semaphore_map(tensor, dp, units, tiles)
    wide = max(head_rows, features)
    vmem = pl.BlockSpec(memory_space=pltpu.VMEM)
    anywhere = pl.BlockSpec(memory_space=pl.ANY)
    args = [pltpu.with_memory_space_constraint(x, pltpu.HBM) for x in (attn, gtop, branch, err, q_t)]
    return pl.pallas_call(
        functools.partial(chain_kernel, (tensor, dp, units, tiles, names)),
        out_shape=(
            pltpu.VMEM((head_rows, width), BF16),
            pltpu.VMEM((tokens, features), BF16),
            pltpu.VMEM((rank, head_rows), F32),
            pltpu.VMEM((head_rows, 2 * rank), BF16),
            pltpu.VMEM((2 * rank, width), BF16),
            pltpu.VMEM((rank, features), F32),
        ),
        in_specs=[anywhere] * 5,
        out_specs=(vmem,) * 6,
        scratch_shapes=[
            pltpu.VMEM((tokens, head_rows), BF16),
            pltpu.VMEM((tokens, features), BF16),
            pltpu.VMEM((tokens, features), BF16),
            pltpu.VMEM((head_rows, width), BF16),
            pltpu.VMEM((rank, features), F32),
            pltpu.VMEM((head_rows, tokens), BF16),
            pltpu.VMEM((tensor, 2 * rank, features), BF16),
            pltpu.VMEM((rank, features), BF16),
            pltpu.VMEM((tensor, tokens, features), BF16),
            pltpu.VMEM((rank, tokens), BF16),
            pltpu.VMEM((rank, tokens), BF16),
            pltpu.VMEM((tensor, rank, tokens), F32),
            pltpu.VMEM((rank, wide), F32),
            pltpu.VMEM((dp, rank, pw), BF16),
            pltpu.VMEM((dp, rank, pw), BF16),
            pltpu.VMEM((dp, rank, pw), BF16),
            pltpu.VMEM((rank, head_rows), BF16),
            pltpu.VMEM((tensor, rank, rank), F32),
            pltpu.VMEM((3 * rank, rank), BF16),
            pltpu.VMEM((tensor, rank, tokens), F32),
            pltpu.VMEM((2 * rank, tokens), BF16),
            pltpu.VMEM((max(1, tensor - 1), rank, features), BF16),
            pltpu.VMEM((tensor, rank, features), BF16),
            pltpu.VMEM((dp, rank, qw), BF16),
            pltpu.VMEM((dp, rank, qw), BF16),
            pltpu.VMEM((tensor, dp, rank, qw), BF16),
            pltpu.SemaphoreType.DMA((count,)),
        ],
        compiler_params=pltpu.CompilerParams(
            collective_id=0, has_side_effects=True, vmem_limit_bytes=43 * 2**20
        ),
        name="chain",
    )(*args)


def finish_kernel(tiles, matrix, grad_in, p, fact, pair, q_own, out, grad_out, p_out, q_out, held, sem):
    head_rows, width = matrix.shape
    tile = head_rows // tiles
    step = min(width, 512)

    def out_copy(i):
        rows = pl.ds(pl.multiple_of(i * tile, tile), tile)
        return pltpu.make_async_copy(held.at[rows], out.at[rows], sem.at[i])

    def row_tile(i, carry):
        rows = pl.ds(pl.multiple_of(i * tile, tile), tile)
        for c in range(width // step):
            here = slice(c * step, (c + 1) * step)
            value = matrix[rows, here].astype(F32) - mm(fact[rows, :], pair[:, here], NN)
            held[rows, here] = value.astype(BF16)
        out_copy(i).start()
        return carry

    small = [
        pltpu.make_async_copy(src, dst, sem.at[tiles + i])
        for i, (src, dst) in enumerate(((grad_in, grad_out), (p, p_out), (q_own, q_out)))
    ]
    for copy in small:
        copy.start()
    lax.fori_loop(0, tiles, row_tile, 0)
    for copy in small:
        copy.wait()

    def landed(i, carry):
        out_copy(i).wait()
        return carry

    lax.fori_loop(0, tiles, landed, 0)


def finish(matrix, grad_in, p, fact, pair, q_own):
    head_rows, width = matrix.shape
    tiles = max(1, head_rows // max(128, head_rows // 16))
    vmem = pl.BlockSpec(memory_space=pltpu.VMEM)
    anywhere = pl.BlockSpec(memory_space=pl.ANY)
    args = [
        pltpu.with_memory_space_constraint(x, pltpu.VMEM)
        for x in (matrix, grad_in, p, fact, pair, q_own)
    ]
    return pl.pallas_call(
        functools.partial(finish_kernel, tiles),
        out_shape=(
            pltpu.HBM(matrix.shape, BF16),
            pltpu.HBM(grad_in.shape, BF16),
            pltpu.HBM(p.shape, F32),
            pltpu.HBM(q_own.shape, F32),
        ),
        in_specs=[vmem] * 6,
        out_specs=(anywhere,) * 4,
        scratch_shapes=[
            pltpu.VMEM((head_rows, width), BF16),
            pltpu.SemaphoreType.DMA((tiles + 3,)),
        ],
        compiler_params=pltpu.CompilerParams(vmem_limit_bytes=20 * 2**20),
        name="finish",
    )(*args)


def on_device(mesh, attn_out, grad_top, branch_grad, error_prev, q_prev):
    micro, rows, features = grad_top.shape
    tokens = micro * rows
    attn = attn_out.reshape(tokens, attn_out.shape[3])
    gtop = grad_top.reshape(tokens, features)
    branch = branch_grad.reshape(tokens, features)
    err = error_prev[0, 0]
    error, grad_in, p, q_own = finish(*chain(mesh, attn, gtop, branch, err, q_prev[0].T))
    return grad_in.reshape(branch_grad.shape), error[None, None], p.T[None], q_own.T[None]


def solution(mesh):
    assert mesh.shape["pipe"] == 2
    return jax.shard_map(
        functools.partial(on_device, mesh),
        mesh=mesh,
        in_specs=(
            P("pipe", None, "dp", "tensor"),
            P(None, "dp", "tensor"),
            P("pipe", None, "dp", "tensor"),
            P("pipe", "dp", "tensor", None),
            P("pipe", "tensor", None),
        ),
        out_specs=(
            P("pipe", None, "dp", "tensor"),
            P("pipe", "dp", "tensor", None),
            P("pipe", "tensor", None),
            P("pipe", "tensor", None),
        ),
        check_vma=False,
    )
```

```python
import functools

import jax
import jax.numpy as jnp
from jax import lax
from jax.experimental import pallas as pl
from jax.experimental.pallas import tpu as pltpu
from jax.sharding import PartitionSpec as P

BF16 = jnp.bfloat16
F32 = jnp.float32
NN = (((1,), (0,)), ((), ()))
NT = (((1,), (1,)), ((), ()))
TN = (((0,), (0,)), ((), ()))


def mm(a, b, dims):
    return lax.dot_general(a, b, dims, preferred_element_type=F32)


def terms(x):
    head = x.astype(BF16)
    tail = (x - head.astype(F32)).astype(BF16)
    return jnp.concatenate([head, tail], axis=0)


def fold(y):
    half = y.shape[0] // 2
    return y[:half] + y[half:]


def add_round(a, b):
    return (a.astype(F32) + b.astype(F32)).astype(BF16)


def inverse_factor(gram):
    rank = gram.shape[0]
    row = lax.broadcasted_iota(jnp.int32, (rank, 2 * rank), 0)
    col = lax.broadcasted_iota(jnp.int32, (rank, 2 * rank), 1)
    work = jnp.concatenate([gram, jnp.where(row == col, 1.0, 0.0)[:, :rank]], axis=1)
    for k in range(rank - 1):
        ratio = work[:, k : k + 1] * (1.0 / work[k : k + 1, k : k + 1])
        work = work - jnp.where(row > k, ratio * work[k : k + 1, :], 0.0)
    diagonal = jnp.sum(jnp.where(row == col, work, 0.0), axis=1, keepdims=True)
    return work[:, rank:] * lax.rsqrt(diagonal)


class Semaphores:
    def __init__(self):
        self.count = 0

    def take(self, n=1):
        first = self.count
        self.count += n
        return first


def semaphore_map(tensor, dp, units, tiles):
    s = Semaphores()
    names = {}
    for name, n in (
        ("err", tiles), ("load", 4),
        ("q_s", tensor), ("q_r", tensor), ("q0_s", 1), ("q0_r", 1),
        ("bulk_s", units), ("bulk_r", units), ("gx_s", 1), ("gx_r", 1),
        ("gq_s", tensor), ("gq_r", tensor), ("p_s", dp), ("p_r", dp),
        ("pg_s", dp), ("pg_r", dp), ("gram_s", tensor), ("gram_r", tensor),
        ("ap_s", tensor), ("ap_r", tensor), ("qx_s", tensor), ("qx_r", tensor),
        ("g_s", tensor * units), ("g_r", tensor * units), ("qp_s", dp), ("qp_r", dp),
        ("qg_s", dp), ("qg_r", dp), ("qf_s", tensor * dp), ("qf_r", tensor * dp),
    ):
        names[name] = s.take(n)
    return names, s.count


def chain_kernel(
    dims, attn_hbm, gtop_hbm, branch_hbm, err_hbm, q_hbm,
    matrix, grad_in, p_out, fact, pair, q_own,
    attn, gtop, branch, err, q_in, at_ref, qg, q0, gbuf, gqx, gqr, gqb, eq,
    psend, prcv, pg, praw, gb, lin, apb, apt, qx, qxr, qsend, qrcv, qf, sem,
):
    tensor, dp, units, tiles, names = dims
    tokens, head_rows = attn.shape
    features = gtop.shape[1]
    rank = q_in.shape[0]
    pw, qw = head_rows // dp, features // dp
    unit = features // units
    shards = unit // qw
    section = lax.axis_index("pipe")
    t = lax.axis_index("tensor")
    r = lax.axis_index("dp")
    scale = 1.0 / tokens

    def at(name, index=0):
        return sem.at[names[name] + index]

    def remote(src, dst, send, recv, **where):
        return pltpu.make_async_remote_copy(
            src_ref=src, dst_ref=dst, send_sem=send, recv_sem=recv,
            device_id=where, device_id_type=pl.DeviceIdType.MESH,
        )

    tensor_peers = [lax.rem(t + o, tensor) for o in range(1, tensor)]
    dp_peers = [lax.rem(r + o, dp) for o in range(1, dp)]

    def over_tensor(src, dst, key):
        return [
            remote(src, dst.at[t], at(key + "_s", o), at(key + "_r", t), tensor=peer)
            for o, peer in enumerate(tensor_peers)
        ]

    def from_tensor(dst, key):
        for peer in tensor_peers:
            remote(dst.at[peer], dst.at[peer], at(key + "_s"), at(key + "_r", peer), tensor=peer).wait_recv()

    def over_dp(src_of, dst, key):
        return [
            remote(src_of(peer), dst.at[r], at(key + "_s", o), at(key + "_r", r), dp=peer)
            for o, peer in enumerate(dp_peers)
        ]

    def from_dp(dst, key):
        for peer in dp_peers:
            remote(dst.at[peer], dst.at[peer], at(key + "_s"), at(key + "_r", peer), dp=peer).wait_recv()

    def start(copies):
        for copy in copies:
            copy.start()

    def sent(copies):
        for copy in copies:
            copy.wait_send()

    late = units // 2

    def place(i):
        return (i + late + 1) % units

    def columns(i):
        return pl.ds(pl.multiple_of(i * unit, unit), unit)

    tile = head_rows // tiles

    def err_copy(i):
        rows = pl.ds(pl.multiple_of(i * tile, tile), tile)
        return pltpu.make_async_copy(err_hbm.at[rows], err.at[rows], at("err", i))

    loads = [
        pltpu.make_async_copy(src, dst, at("load", i))
        for i, (src, dst) in enumerate(
            ((q_hbm, q_in), (branch_hbm, branch), (gtop_hbm, gtop), (attn_hbm, attn))
        )
    ]
    start(loads)
    for i in range(tiles):
        err_copy(i).start()

    barrier = pltpu.get_barrier_semaphore()
    for peer in tensor_peers:
        pl.semaphore_signal(barrier, inc=1, device_id={"tensor": peer}, device_id_type=pl.DeviceIdType.MESH)
    for peer in dp_peers:
        pl.semaphore_signal(barrier, inc=1, device_id={"dp": peer}, device_id_type=pl.DeviceIdType.MESH)
    pl.semaphore_signal(barrier, inc=1, device_id={"pipe": 1 - section}, device_id_type=pl.DeviceIdType.MESH)
    loads[0].wait()
    qg[t] = terms(q_in[...])
    loads[1].wait()
    pl.semaphore_wait(barrier, tensor + dp - 1)

    q0_copy = remote(qg.at[t, pl.ds(0, rank)], q0, at("q0_s"), at("q0_r"), pipe=1 - section)
    gx_copy = remote(gqx, gqr, at("gx_s"), at("gx_r"), pipe=1 - section)
    ahead = units // 4

    def bulk_copy(i):
        return remote(branch.at[:, columns(i)], gbuf.at[t, :, columns(i)], at("bulk_s", i), at("bulk_r", i), pipe=1 - section)

    @pl.when(section == 0)
    def _():
        q0_copy.start()

    @pl.when(section == 1)
    def _():
        for i in range(ahead):
            bulk_copy(place(i)).start()

    q_copies = over_tensor(qg.at[t], qg, "q")
    start(q_copies)
    loads[2].wait()
    loads[3].wait()

    @pl.when(section == 1)
    def _():
        grad_in[...] = add_round(gtop[...], branch[...])
        gqb[t] = fold(mm(qg[t], gtop[...], NT)) * scale

    from_tensor(qg, "q")

    def eq_tile(i, carry):
        err_copy(i).wait()
        rows = pl.ds(pl.multiple_of(i * tile, tile), tile)
        total = mm(qg[0], err[rows, pl.ds(0, features)], NT)
        for tt in range(1, tensor):
            total += mm(qg[tt], err[rows, pl.ds(tt * features, features)], NT)
        eq[:, rows] = fold(total)
        return carry

    lax.fori_loop(0, tiles, eq_tile, 0)

    @pl.when(section == 1)
    def _():
        q0_copy.wait_recv()
        gqx[...] = (mm(q0[...], grad_in[...], NT) * scale).astype(BF16)
        gx_copy.start()
        for i in range(ahead, units):
            bulk_copy(place(i)).start()

    @pl.when(section == 0)
    def _():
        gx_copy.wait_recv()
        gqb[t] = gqr[...].astype(F32)

    gq_copies = over_tensor(gqb.at[t], gqb, "gq")
    start(gq_copies)
    from_tensor(gqb, "gq")
    gq = gqb[0]
    for tt in range(1, tensor):
        gq += gqb[tt]
    p_local = (fold(mm(terms(gq), attn[...], NN)) + eq[:, :head_rows]).astype(BF16)
    for j in range(dp):
        psend[j] = p_local[:, j * pw : (j + 1) * pw]
    p_copies = over_dp(lambda peer: psend.at[peer], prcv, "p")
    start(p_copies)

    def g_copies(i):
        here = gbuf.at[t, :, columns(i)]
        return [
            remote(here, here, at("g_s", o * units + i), at("g_r", t * units + i), tensor=peer)
            for o, peer in enumerate(tensor_peers)
        ]

    def land_unit(i, carry):
        i = place(i)
        cols = columns(i)

        @pl.when(section == 0)
        def _():
            bulk_copy(i).wait_recv()
            out_grad = add_round(gtop[:, cols], gbuf[t, :, cols])
            gbuf[t, :, cols] = out_grad
            grad_in[:, cols] = add_round(out_grad, branch[:, cols])

        @pl.when(section == 1)
        def _():
            gbuf[t, :, cols] = gtop[:, cols]

        start(g_copies(i))
        return carry

    def matrix_unit(i, carry):
        i = place(i)
        cols = columns(i)
        for peer in tensor_peers:
            here = gbuf.at[peer, :, cols]
            remote(here, here, at("g_s"), at("g_r", peer * units + i), tensor=peer).wait_recv()
        block = min(head_rows, 512)
        for tt in range(tensor):
            there = pl.ds(pl.multiple_of(tt * features + i * unit, unit), unit)
            grads = gbuf[tt, :, cols]
            for c in range(head_rows // block):
                rows = pl.ds(c * block, block)
                value = mm(at_ref[rows, :], grads, NN) * scale + err[rows, there].astype(F32)
                matrix[rows, there] = value.astype(BF16)
        return carry

    def transpose_tile(i, carry):
        rows = pl.ds(pl.multiple_of(i * tile, tile), tile)
        at_ref[rows, :] = attn[:, rows].T
        return carry

    first, second, third = units // 4, 3 * units // 8, 5 * units // 8
    lax.fori_loop(0, tiles, transpose_tile, 0)
    lax.fori_loop(0, first, land_unit, 0)
    lax.fori_loop(0, first, matrix_unit, 0)
    from_dp(prcv, "p")
    total = psend[r].astype(F32)
    for peer in dp_peers:
        total += prcv[peer].astype(F32)
    pg[r] = (total * (1.0 / dp)).astype(BF16)
    pg_copies = over_dp(lambda peer: pg.at[r], pg, "pg")
    start(pg_copies)
    lax.fori_loop(first, second, land_unit, 0)
    lax.fori_loop(first, second, matrix_unit, 0)
    from_dp(pg, "pg")
    for j in range(dp):
        praw[:, j * pw : (j + 1) * pw] = pg[j]

    gb[t] = mm(praw[...], praw[...], NT)
    gram_copies = over_tensor(gb.at[t], gb, "gram")
    start(gram_copies)
    apb[t] = mm(praw[...], attn[...], NT) * scale
    ap_copies = over_tensor(apb.at[t], apb, "ap")
    start(ap_copies)

    step = min(features, 512)

    def project(owner, done):
        def column(i, carry):
            here = pl.ds(pl.multiple_of(i * step, step), step)
            there = pl.ds(pl.multiple_of(owner * features + i * step, step), step)
            done(here, mm(praw[...], err[:, there], NN))
            return carry

        lax.fori_loop(0, features // step, column, 0)

    qx_copies = []
    for o, peer in enumerate(tensor_peers):
        def keep(here, value, slot=o):
            qx[slot, :, here] = value.astype(BF16)

        project(peer, keep)
        copy = remote(qx.at[o], qxr.at[t], at("qx_s", o), at("qx_r", t), tensor=peer)
        copy.start()
        qx_copies.append(copy)

    def keep_own(here, value):
        eq[:, here] = value

    project(t, keep_own)
    lax.fori_loop(second, third, land_unit, 0)
    from_tensor(apb, "ap")
    ap = apb[0]
    for tt in range(1, tensor):
        ap += apb[tt]
    apt[...] = terms(ap)
    from_tensor(qxr, "qx")

    def q_copy(j):
        return remote(qsend.at[j], qrcv.at[r], at("qp_s", j), at("qp_r", r), dp=j)

    def q_unit(i, carry):
        i = place(i)
        cols = columns(i)
        value = eq[:, cols] + fold(mm(apt[...], gbuf[t, :, cols], NN))
        for peer in tensor_peers:
            value += qxr[peer, :, cols].astype(F32)
        value = value.astype(BF16)
        for k in range(shards):
            j = i * shards + k
            qsend[j] = value[:, k * qw : (k + 1) * qw]

            @pl.when(j != r)
            def _():
                q_copy(j).start()

        return carry

    def qg_copies():
        return [
            remote(qf.at[t, r], qf.at[t, r], at("qg_s", o), at("qg_r", r), dp=peer)
            for o, peer in enumerate(dp_peers)
        ]

    def forward(j):
        return [
            remote(qf.at[t, j], qf.at[t, j], at("qf_s", o * dp + j), at("qf_r", t * dp + j), tensor=peer)
            for o, peer in enumerate(tensor_peers)
        ]

    def reduce_q():
        from_dp(qrcv, "qp")
        total = qsend[r].astype(F32)
        for peer in dp_peers:
            total += qrcv[peer].astype(F32)
        qf[t, r] = (total * (1.0 / dp)).astype(BF16)
        start(qg_copies())
        start(forward(r))

    lax.fori_loop(0, third, q_unit, 0)

    from_tensor(gb, "gram")
    gram = gb[0]
    for tt in range(1, tensor):
        gram += gb[tt]
    inverse = inverse_factor(gram)
    head = inverse.astype(BF16)
    rest = inverse - head.astype(F32)
    middle = rest.astype(BF16)
    last = (rest - middle.astype(F32)).astype(BF16)
    lin[...] = jnp.concatenate([head, middle, last], axis=0)

    def applied(rows):
        parts = mm(lin[...], rows, NN)
        return parts[:rank] + (parts[rank : 2 * rank] + parts[2 * rank :])


    def late_unit(i, carry):
        land_unit(i, 0)
        return q_unit(i, carry)

    lax.fori_loop(third, units - 1, late_unit, 0)
    p = applied(praw[...])
    p_out[...] = p
    fact[...] = terms(p).T
    middle_unit = min(units - 1, second + 2)
    lax.fori_loop(second, middle_unit, matrix_unit, 0)

    @pl.when(r // shards != late)
    def _():
        reduce_q()

    late_unit(units - 1, 0)
    later_unit = min(units, middle_unit + 2)
    lax.fori_loop(middle_unit, later_unit, matrix_unit, 0)

    @pl.when(r // shards == late)
    def _():
        reduce_q()

    order = [(j + (late + 1) * shards) % dp for j in range(dp)]

    def gather_q(owners):
        for j in owners:
            @pl.when(r != j)
            def _(j=j):
                remote(qf.at[t, j], qf.at[t, j], at("qg_s"), at("qg_r", j), dp=j).wait_recv()
                start(forward(j))

        for j in owners:
            q_own[:, j * qw : (j + 1) * qw] = applied(qf[t, j])
        for peer in tensor_peers:
            for j in owners:
                remote(qf.at[peer, j], qf.at[peer, j], at("qf_s"), at("qf_r", peer * dp + j), tensor=peer).wait_recv()
        for tt in range(tensor):
            for j in owners:
                begin = tt * features + j * qw
                value = applied(qf[tt, j]).astype(BF16)
                pair[:rank, begin : begin + qw] = value
                pair[rank:, begin : begin + qw] = value

    gather_q(order[: dp - shards])
    lax.fori_loop(later_unit, units, matrix_unit, 0)
    gather_q(order[dp - shards :])

    @pl.when(section == 0)
    def _():
        q0_copy.wait_send()

    @pl.when(section == 1)
    def _():
        gx_copy.wait_send()
        for i in range(units):
            bulk_copy(i).wait_send()

    for copies in (q_copies, gq_copies, p_copies, pg_copies, gram_copies, ap_copies,
                   qx_copies, qg_copies()):
        sent(copies)

    def rows_sent(j, carry):
        sent(forward(j))

        @pl.when(j != r)
        def _():
            q_copy(j).wait_send()

        return carry

    lax.fori_loop(0, dp, rows_sent, 0)

    def g_sent(i, carry):
        sent(g_copies(i))
        return carry

    lax.fori_loop(0, units, g_sent, 0)


def chain(mesh, attn, gtop, branch, err, q_t):
    tensor, dp = mesh.shape["tensor"], mesh.shape["dp"]
    tokens, head_rows = attn.shape
    features = gtop.shape[1]
    rank = q_t.shape[0]
    tiles = max(1, head_rows // max(128, head_rows // 8))
    width = tensor * features
    pw, qw = head_rows // dp, features // dp
    units = features // max(128, features // 8, qw)
    names, count = semaphore_map(tensor, dp, units, tiles)
    wide = max(head_rows, features)
    vmem = pl.BlockSpec(memory_space=pltpu.VMEM)
    anywhere = pl.BlockSpec(memory_space=pl.ANY)
    args = [pltpu.with_memory_space_constraint(x, pltpu.HBM) for x in (attn, gtop, branch, err, q_t)]
    return pl.pallas_call(
        functools.partial(chain_kernel, (tensor, dp, units, tiles, names)),
        out_shape=(
            pltpu.VMEM((head_rows, width), BF16),
            pltpu.VMEM((tokens, features), BF16),
            pltpu.VMEM((rank, head_rows), F32),
            pltpu.VMEM((head_rows, 2 * rank), BF16),
            pltpu.VMEM((2 * rank, width), BF16),
            pltpu.VMEM((rank, features), F32),
        ),
        in_specs=[anywhere] * 5,
        out_specs=(vmem,) * 6,
        scratch_shapes=[
            pltpu.VMEM((tokens, head_rows), BF16),
            pltpu.VMEM((tokens, features), BF16),
            pltpu.VMEM((tokens, features), BF16),
            pltpu.VMEM((head_rows, width), BF16),
            pltpu.VMEM((rank, features), F32),
            pltpu.VMEM((head_rows, tokens), BF16),
            pltpu.VMEM((tensor, 2 * rank, features), BF16),
            pltpu.VMEM((rank, features), BF16),
            pltpu.VMEM((tensor, tokens, features), BF16),
            pltpu.VMEM((rank, tokens), BF16),
            pltpu.VMEM((rank, tokens), BF16),
            pltpu.VMEM((tensor, rank, tokens), F32),
            pltpu.VMEM((rank, wide), F32),
            pltpu.VMEM((dp, rank, pw), BF16),
            pltpu.VMEM((dp, rank, pw), BF16),
            pltpu.VMEM((dp, rank, pw), BF16),
            pltpu.VMEM((rank, head_rows), BF16),
            pltpu.VMEM((tensor, rank, rank), F32),
            pltpu.VMEM((3 * rank, rank), BF16),
            pltpu.VMEM((tensor, rank, tokens), F32),
            pltpu.VMEM((2 * rank, tokens), BF16),
            pltpu.VMEM((max(1, tensor - 1), rank, features), BF16),
            pltpu.VMEM((tensor, rank, features), BF16),
            pltpu.VMEM((dp, rank, qw), BF16),
            pltpu.VMEM((dp, rank, qw), BF16),
            pltpu.VMEM((tensor, dp, rank, qw), BF16),
            pltpu.SemaphoreType.DMA((count,)),
        ],
        compiler_params=pltpu.CompilerParams(
            collective_id=0, has_side_effects=True, vmem_limit_bytes=43 * 2**20
        ),
        name="chain",
    )(*args)


def finish_kernel(tiles, matrix, grad_in, p, fact, pair, q_own, out, grad_out, p_out, q_out, held, sem):
    head_rows, width = matrix.shape
    tile = head_rows // tiles
    step = min(width, 512)

    def out_copy(i):
        rows = pl.ds(pl.multiple_of(i * tile, tile), tile)
        return pltpu.make_async_copy(held.at[rows], out.at[rows], sem.at[i])

    def row_tile(i, carry):
        rows = pl.ds(pl.multiple_of(i * tile, tile), tile)
        for c in range(width // step):
            here = slice(c * step, (c + 1) * step)
            value = matrix[rows, here].astype(F32) - mm(fact[rows, :], pair[:, here], NN)
            held[rows, here] = value.astype(BF16)
        out_copy(i).start()
        return carry

    small = [
        pltpu.make_async_copy(src, dst, sem.at[tiles + i])
        for i, (src, dst) in enumerate(((grad_in, grad_out), (p, p_out), (q_own, q_out)))
    ]
    for copy in small:
        copy.start()
    lax.fori_loop(0, tiles, row_tile, 0)
    for copy in small:
        copy.wait()

    def landed(i, carry):
        out_copy(i).wait()
        return carry

    lax.fori_loop(0, tiles, landed, 0)


def finish(matrix, grad_in, p, fact, pair, q_own):
    head_rows, width = matrix.shape
    tiles = max(1, head_rows // max(128, head_rows // 16))
    vmem = pl.BlockSpec(memory_space=pltpu.VMEM)
    anywhere = pl.BlockSpec(memory_space=pl.ANY)
    args = [
        pltpu.with_memory_space_constraint(x, pltpu.VMEM)
        for x in (matrix, grad_in, p, fact, pair, q_own)
    ]
    return pl.pallas_call(
        functools.partial(finish_kernel, tiles),
        out_shape=(
            pltpu.HBM(matrix.shape, BF16),
            pltpu.HBM(grad_in.shape, BF16),
            pltpu.HBM(p.shape, F32),
            pltpu.HBM(q_own.shape, F32),
        ),
        in_specs=[vmem] * 6,
        out_specs=(anywhere,) * 4,
        scratch_shapes=[
            pltpu.VMEM((head_rows, width), BF16),
            pltpu.SemaphoreType.DMA((tiles + 3,)),
        ],
        compiler_params=pltpu.CompilerParams(vmem_limit_bytes=20 * 2**20),
        name="finish",
    )(*args)


def on_device(mesh, attn_out, grad_top, branch_grad, error_prev, q_prev):
    micro, rows, features = grad_top.shape
    tokens = micro * rows
    attn = attn_out.reshape(tokens, attn_out.shape[3])
    gtop = grad_top.reshape(tokens, features)
    branch = branch_grad.reshape(tokens, features)
    err = error_prev[0, 0]
    error, grad_in, p, q_own = finish(*chain(mesh, attn, gtop, branch, err, q_prev[0].T))
    return grad_in.reshape(branch_grad.shape), error[None, None], p.T[None], q_own.T[None]


def solution(mesh):
    assert mesh.shape["pipe"] == 2
    return jax.shard_map(
        functools.partial(on_device, mesh),
        mesh=mesh,
        in_specs=(
            P("pipe", None, "dp", "tensor"),
            P(None, "dp", "tensor"),
            P("pipe", None, "dp", "tensor"),
            P("pipe", "dp", "tensor", None),
            P("pipe", "tensor", None),
        ),
        out_specs=(
            P("pipe", None, "dp", "tensor"),
            P("pipe", "dp", "tensor", None),
            P("pipe", "tensor", None),
            P("pipe", "tensor", None),
        ),
        check_vma=False,
    )
```
